8 devices in a mesh: dp: 1 (over z), cp: 8 (over y, x, core).
Axes of the slice: x: 2, y: 2, z: 1, core: 2. Of those that a mesh axis runs over, the one named last changes fastest.
Arguments:
- hidden: bfloat16 [16, 2048, 5120], P('dp', 'cp')
- positions: int32 [16, 2048], P('dp', 'cp')
- w_q: bfloat16 [5120, 32, 128], replicated
- w_k: bfloat16 [5120, 8, 128], replicated
- w_v: bfloat16 [5120, 8, 128], replicated
- w_o: bfloat16 [32, 128, 5120], replicated
Outputs:
- output: bfloat16 [16, 2048, 5120], P('dp', 'cp')
All inputs are finite; a program needn't handle non-finite values.
Results may differ from the reference program's by a relative error of at most 0.00865.
Values are sent between devices in bfloat16 or wider.
A program may use at most 1 GiB of HBM per device.

```python
import jax
import jax.numpy as jnp
from jax import lax

BATCH = 16
SEQ = 2048
D = 5120
HEADS = 32
KV_HEADS = 8
HEAD = 128

ROPE_BASE = 500000.0
Q_PER_KV = HEADS // KV_HEADS


def setup_inputs(seed: int = 0, part: int = 0) -> dict:
    part_key = jax.random.fold_in(jax.random.key(seed), part)
    k_noise, k_coef, k_phase, k_step, k_first = jax.random.split(part_key, 5)
    k_wq, k_wk, k_wv, k_wo = jax.random.split(jax.random.key(seed + 1), 4)
    time_grid = jnp.arange(SEQ, dtype=jnp.float32) / SEQ
    mode_ids = jnp.arange(1, 5, dtype=jnp.float32)
    phases = jax.random.uniform(k_phase, (BATCH, 4), jnp.float32, 0.0, 6.2831853)
    wave_vals = jnp.cos(6.2831853 * time_grid[None, :, None] * mode_ids[None, None, :] + phases[:, None, :])
    mode_coef = 0.6 * jax.random.normal(k_coef, (BATCH, 4, D), jnp.float32)
    slow_part = jnp.einsum('bsm,bmd->bsd', wave_vals, mode_coef)
    noise_part = 0.6 * jax.random.normal(k_noise, (BATCH, SEQ, D), jnp.float32)
    hidden = (slow_part + noise_part).astype(jnp.bfloat16)
    step_sizes = jax.random.randint(k_step, (BATCH, SEQ), 1, 5)
    first_pos = jax.random.randint(k_first, (BATCH, 1), 0, 4)
    positions = (first_pos + jnp.cumsum(step_sizes, axis=1) - step_sizes[:, :1]).astype(jnp.int32)
    w_q = (jax.random.normal(k_wq, (D, HEADS, HEAD), jnp.float32) * D ** -0.5).astype(jnp.bfloat16)
    w_k = (jax.random.normal(k_wk, (D, KV_HEADS, HEAD), jnp.float32) * D ** -0.5).astype(jnp.bfloat16)
    w_v = (jax.random.normal(k_wv, (D, KV_HEADS, HEAD), jnp.float32) * (2.0 * D ** -0.5)).astype(jnp.bfloat16)
    w_o = (jax.random.normal(k_wo, (HEADS, HEAD, D), jnp.float32) * (HEADS * HEAD) ** -0.5).astype(jnp.bfloat16)
    return {'hidden': hidden, 'positions': positions, 'w_q': w_q, 'w_k': w_k, 'w_v': w_v, 'w_o': w_o}


def rope_tables(positions):
    inv_freq = ROPE_BASE ** (-jnp.arange(0, HEAD, 2, dtype=jnp.float32) / HEAD)
    angles = positions.astype(jnp.float32)[..., None] * inv_freq
    angles = jnp.concatenate([angles, angles], axis=-1)
    return jnp.cos(angles)[:, :, None, :], jnp.sin(angles)[:, :, None, :]


def rope_apply(in_vals, cos_tab, sin_tab):
    half_dim = in_vals.shape[-1] // 2
    val_f32 = in_vals.astype(jnp.float32)
    rotated = jnp.concatenate([-val_f32[..., half_dim:], val_f32[..., :half_dim]], axis=-1)
    return (val_f32 * cos_tab + rotated * sin_tab).astype(jnp.bfloat16)


def reference(hidden, positions, w_q, w_k, w_v, w_o):
    x_float = hidden.astype(jnp.float32)
    queries = jnp.einsum('bsd,dhe->bshe', x_float, w_q.astype(jnp.float32)).astype(jnp.bfloat16)
    k_proj = jnp.einsum('bsd,dhe->bshe', x_float, w_k.astype(jnp.float32)).astype(jnp.bfloat16)
    values = jnp.einsum('bsd,dhe->bshe', x_float, w_v.astype(jnp.float32)).astype(jnp.bfloat16)
    cos_tab, sin_tab = rope_tables(positions)
    queries = rope_apply(queries, cos_tab, sin_tab)
    k_rot = rope_apply(k_proj, cos_tab, sin_tab)
    q_block = 16
    n_blocks = SEQ // q_block
    q_blocks = queries.reshape(BATCH, n_blocks, q_block, KV_HEADS, Q_PER_KV, HEAD).transpose(1, 0, 2, 3, 4, 5)
    pos_blocks = positions.reshape(BATCH, n_blocks, q_block).transpose(1, 0, 2)
    k_float = k_rot.astype(jnp.float32)
    v_float = values.astype(jnp.float32)
    sm_scale = HEAD ** -0.5

    def one_block(block_args):
        q_blk, pos_blk = block_args
        scores = jnp.einsum('bqkge,bske->bkgqs', q_blk.astype(jnp.float32), k_float) * sm_scale
        allowed = positions[:, None, None, None, :] <= pos_blk[:, None, None, :, None]
        scores = jnp.where(allowed, scores, -jnp.inf)
        row_max = jnp.max(scores, axis=-1, keepdims=True)
        p_weights = jnp.exp(scores - row_max)
        row_sum = jnp.sum(p_weights, axis=-1)
        out_acc = jnp.einsum('bkgqs,bske->bqkge', p_weights.astype(jnp.bfloat16).astype(jnp.float32), v_float)
        return (out_acc / row_sum.transpose(0, 3, 1, 2)[..., None]).astype(jnp.bfloat16)

    attn_blocks = lax.map(one_block, (q_blocks, pos_blocks))
    attn_out = attn_blocks.transpose(1, 0, 2, 3, 4, 5).reshape(BATCH, SEQ, HEADS, HEAD)
    proj_out = jnp.einsum('bshe,hed->bsd', attn_out.astype(jnp.float32), w_o.astype(jnp.float32))
    return (x_float + proj_out).astype(jnp.bfloat16)
```

```python
import functools

import jax
import jax.numpy as jnp
from jax import lax
from jax.experimental import pallas as pl
from jax.experimental.pallas import tpu as pltpu
from jax.sharding import PartitionSpec as P

ROPE_BASE = 500000.0
HEAD = 128
LOG2E = 1.4426950408889634
VMEM_LIMIT = 60 * 1024 * 1024
CHUNKS = (4, 4, 4, 4)


def rope_tables(positions):
    inv_freq = ROPE_BASE ** (-jnp.arange(0, HEAD, 2, dtype=jnp.float32) / HEAD)
    angles = positions.astype(jnp.float32).reshape(-1, 1) * inv_freq
    cos, sin = jnp.cos(angles), jnp.sin(angles)
    return jnp.concatenate([cos, cos], axis=-1), jnp.concatenate([-sin, sin], axis=-1)


def rope_round(vals, cos, sin):
    vals = vals.astype(jnp.bfloat16).astype(jnp.float32)
    return (vals * cos + pltpu.roll(vals, HEAD // 2, 1) * sin).astype(jnp.bfloat16)


def q_kernel(x_ref, w_ref, cos_ref, sin_ref, o_ref):
    rows, width = o_ref.shape
    step = 512

    @pl.loop(0, rows // step)
    def _(r):
        at = pl.ds(pl.multiple_of(r * step, step), step)
        x = x_ref[at, :]
        cos, sin = cos_ref[at, :], sin_ref[at, :]
        for c in range(0, width, 256):
            acc = jnp.dot(x, w_ref[:, c:c + 256], preferred_element_type=jnp.float32)
            o_ref[at, c:c + HEAD] = rope_round(acc[:, :HEAD], cos, sin)
            o_ref[at, c + HEAD:c + 256] = rope_round(acc[:, HEAD:], cos, sin)


def project_q(x, w, cos, sin, tile_m=1024, tile_n=512):
    m, d = x.shape
    n = w.shape[1]
    return pl.pallas_call(
        q_kernel,
        out_shape=jax.ShapeDtypeStruct((m, n), jnp.bfloat16),
        grid=(m // tile_m, n // tile_n),
        in_specs=[
            pl.BlockSpec((tile_m, d), lambda i, j: (i, 0)),
            pl.BlockSpec((d, tile_n), lambda i, j: (0, j)),
            pl.BlockSpec((tile_m, HEAD), lambda i, j: (i, 0)),
            pl.BlockSpec((tile_m, HEAD), lambda i, j: (i, 0)),
        ],
        out_specs=pl.BlockSpec((tile_m, tile_n), lambda i, j: (i, j)),
        compiler_params=pltpu.CompilerParams(vmem_limit_bytes=VMEM_LIMIT),
        cost_estimate=pl.CostEstimate(flops=2 * m * n * d, bytes_accessed=2 * (m * d + m * n + 4 * n * d), transcendentals=0),
        name="project_q",
    )(x, w, cos, sin)


def kv_kernel(x_ref, wk_ref, wv_ref, cos_ref, sin_ref, k_ref, v_ref):
    seqs, tok = v_ref.shape[0], v_ref.shape[2]

    @pl.loop(0, seqs)
    def _(s):
        at = pl.ds(pl.multiple_of(s * tok, tok), tok)
        x = x_ref[at, :]
        cos, sin = cos_ref[at, :], sin_ref[at, :]
        for c in range(0, wk_ref.shape[1], 256):
            acc = jnp.dot(x, wk_ref[:, c:c + 256], preferred_element_type=jnp.float32)
            k_ref[s, :, c:c + HEAD] = rope_round(acc[:, :HEAD], cos, sin)
            k_ref[s, :, c + HEAD:c + 256] = rope_round(acc[:, HEAD:], cos, sin)
            acc = jnp.dot(x, wv_ref[:, c:c + 256], preferred_element_type=jnp.float32)
            v_ref[s, c:c + 256, :] = acc.T.astype(jnp.bfloat16)


def project_kv(x, w_k, w_v, cos, sin, seq0, seqs, tok, tile_n=256):
    d, n = w_k.shape
    rows = seqs * tok
    assert seq0 % seqs == 0
    i0 = seq0 // seqs
    return pl.pallas_call(
        kv_kernel,
        out_shape=(
            jax.ShapeDtypeStruct((seqs, tok, n), jnp.bfloat16),
            jax.ShapeDtypeStruct((seqs, n, tok), jnp.bfloat16),
        ),
        grid=(n // tile_n,),
        in_specs=[
            pl.BlockSpec((rows, d), lambda j: (i0, 0)),
            pl.BlockSpec((d, tile_n), lambda j: (0, j)),
            pl.BlockSpec((d, tile_n), lambda j: (0, j)),
            pl.BlockSpec((rows, HEAD), lambda j: (i0, 0)),
            pl.BlockSpec((rows, HEAD), lambda j: (i0, 0)),
        ],
        out_specs=(
            pl.BlockSpec((seqs, tok, tile_n), lambda j: (0, 0, j)),
            pl.BlockSpec((seqs, tile_n, tok), lambda j: (0, j, 0)),
        ),
        compiler_params=pltpu.CompilerParams(vmem_limit_bytes=VMEM_LIMIT),
        cost_estimate=pl.CostEstimate(flops=4 * rows * n * d, bytes_accessed=2 * rows * d + 4 * n * d + 4 * rows * n, transcendentals=0),
        name="project_kv",
    )(x, w_k, w_v, cos, sin)


def attn_kernel(me_ref, q_ref, k_ref, v_ref, *rest):
    o_ref, s_even, s_odd = rest[-3:]
    me = me_ref[0]
    tok = q_ref.shape[1]
    heads = q_ref.shape[2] // HEAD
    scale = HEAD ** -0.5 * LOG2E
    bufs = (s_even, s_odd)

    def scores(h, blocks, first_masked):
        buf = bufs[h % 2]
        q = q_ref[0, :, h * HEAD:(h + 1) * HEAD]
        top = jnp.full((8, tok), -jnp.inf, jnp.float32)
        for j in range(blocks):
            s = lax.dot_general(k_ref[j, 0], q, (((1,), (1,)), ((), ())), preferred_element_type=jnp.float32)
            if j >= first_masked:
                key = lax.broadcasted_iota(jnp.int32, (tok, tok), 0) + j * tok
                row = lax.broadcasted_iota(jnp.int32, (tok, tok), 1) + me * tok
                s = jnp.where(key <= row, s, -jnp.inf)
            buf[j * tok:(j + 1) * tok, :] = s
            top = jnp.maximum(top, jnp.max(s.reshape(tok // 8, 8, tok), axis=0))
        return jnp.max(top, axis=0, keepdims=True)

    def apply(h, blocks, top):
        buf = bufs[h % 2]
        shift = top * scale
        total = jnp.zeros((8, tok), jnp.float32)
        acc = None
        for j in range(blocks):
            p = jnp.exp2(buf[j * tok:(j + 1) * tok, :] * scale - shift)
            total = total + jnp.sum(p.reshape(tok // 8, 8, tok), axis=0)
            part = jnp.dot(v_ref[j, 0], p.astype(jnp.bfloat16), preferred_element_type=jnp.float32)
            acc = part if acc is None else acc + part
        out = acc * (1.0 / jnp.sum(total, axis=0, keepdims=True))
        o_ref[0, :, h * HEAD:(h + 1) * HEAD] = out.T.astype(jnp.bfloat16)

    def run(blocks, first_masked):
        tops = []
        for h in range(heads + 1):
            if h < heads:
                tops.append(scores(h, blocks, first_masked))
            if h > 0:
                apply(h - 1, blocks, tops[h - 1])

    n_dev = k_ref.shape[0]
    for pair in range(n_dev // 2):
        @pl.when(me // 2 == pair)
        def _():
            run(2 * pair + 2, 2 * pair)


def attention(me, q, k_all, v_all, seq0, after):
    n_dev, seqs, tok, kv_width = k_all.shape
    n_kv = kv_width // HEAD
    width = q.shape[2] // n_kv
    flops = 4 * seqs * tok * n_dev * tok * q.shape[2]
    return pl.pallas_call(
        attn_kernel,
        out_shape=jax.ShapeDtypeStruct((seqs, tok, q.shape[2]), jnp.bfloat16),
        grid_spec=pltpu.PrefetchScalarGridSpec(
            num_scalar_prefetch=1,
            grid=(seqs, n_kv),
            in_specs=[
                pl.BlockSpec((1, tok, width), lambda b, g, me: (b + seq0 if seq0 else b, 0, g)),
                pl.BlockSpec((n_dev, 1, tok, HEAD), lambda b, g, me: (0, b, 0, g)),
                pl.BlockSpec((n_dev, 1, HEAD, tok), lambda b, g, me: (0, b, g, 0)),
            ] + [pl.BlockSpec(memory_space=pl.ANY)] * len(after),
            out_specs=pl.BlockSpec((1, tok, width), lambda b, g, me: (b, 0, g)),
            scratch_shapes=[pltpu.VMEM((n_dev * tok, tok), jnp.float32)] * 2,
        ),
        compiler_params=pltpu.CompilerParams(vmem_limit_bytes=VMEM_LIMIT),
        cost_estimate=pl.CostEstimate(flops=flops, bytes_accessed=4 * k_all.size + 4 * seqs * tok * q.shape[2], transcendentals=0),
        name="attention",
    )(me, q, k_all, v_all, *after)


def o_kernel(o_ref, w_ref, x_ref, *rest):
    y_ref = rest[-1]
    rows = o_ref.shape[0]
    step = 512

    @pl.loop(0, rows // step)
    def _(r):
        at = pl.ds(pl.multiple_of(r * step, step), step)
        a = o_ref[at, :]
        for c in range(0, w_ref.shape[1], 256):
            acc = jnp.dot(a, w_ref[:, c:c + 256], preferred_element_type=jnp.float32)
            y_ref[at, c:c + 256] = (x_ref[at, c:c + 256].astype(jnp.float32) + acc).astype(jnp.bfloat16)


def project_o(o, w, x, y, row0, tile_n=512):
    rows, n_in = o.shape
    m, d = x.shape
    assert row0 % rows == 0
    i0 = row0 // rows
    specs = [
        pl.BlockSpec((rows, n_in), lambda j: (0, 0)),
        pl.BlockSpec((n_in, tile_n), lambda j: (0, j)),
        pl.BlockSpec((rows, tile_n), lambda j: (i0, j)),
    ]
    args = [o, w, x]
    alias = {}
    if y is not None:
        specs.append(pl.BlockSpec(memory_space=pl.ANY))
        args.append(y)
        alias = {3: 0}
    return pl.pallas_call(
        o_kernel,
        out_shape=jax.ShapeDtypeStruct((m, d), jnp.bfloat16),
        grid=(d // tile_n,),
        in_specs=specs,
        out_specs=pl.BlockSpec((rows, tile_n), lambda j: (i0, j)),
        input_output_aliases=alias,
        compiler_params=pltpu.CompilerParams(vmem_limit_bytes=VMEM_LIMIT),
        cost_estimate=pl.CostEstimate(flops=2 * rows * n_in * d, bytes_accessed=2 * (n_in * d + rows * n_in + 2 * rows * d), transcendentals=0),
        name="project_o",
    )(*args)


def solution(mesh):
    def per_device(hidden, positions, w_q, w_k, w_v, w_o):
        seqs, tok, d = hidden.shape
        x = hidden.reshape(seqs * tok, d)
        w_q = w_q.reshape(d, -1)
        w_k = w_k.reshape(d, -1)
        w_v = w_v.reshape(d, -1)
        w_o = w_o.reshape(-1, d)
        cos, sin = rope_tables(positions)
        me = lax.axis_index('cp').astype(jnp.int32).reshape(1)
        gathered = []
        seq0 = 0
        for n in CHUNKS:
            k, v = project_kv(x, w_k, w_v, cos, sin, seq0, n, tok)
            gathered.append((lax.all_gather(k, 'cp', axis=0), lax.all_gather(v, 'cp', axis=0)))
            seq0 += n
        q = project_q(x, w_q, cos, sin).reshape(seqs, tok, -1)
        y = None
        seq0 = 0
        for n, (k_all, v_all) in zip(CHUNKS, gathered):
            o = attention(me, q, k_all, v_all, seq0, () if y is None else (y,))
            y = project_o(o.reshape(n * tok, -1), w_o, x, y, seq0 * tok)
            seq0 += n
        return y.reshape(seqs, tok, d)

    rep_spec = P(None, None, None)
    return jax.shard_map(per_device, mesh=mesh, in_specs=(P('dp', 'cp', None), P('dp', 'cp'), rep_spec, rep_spec, rep_spec, rep_spec), out_specs=P('dp', 'cp', None), check_vma=False)
```

```python
import functools

import jax
import jax.numpy as jnp
from jax import lax
from jax.experimental import pallas as pl
from jax.experimental.pallas import tpu as pltpu
from jax.sharding import PartitionSpec as P

ROPE_BASE = 500000.0
HEAD = 128
LOG2E = 1.4426950408889634
VMEM_LIMIT = 60 * 1024 * 1024
CHUNKS = (4, 4, 4, 4)


def rope_tables(positions):
    inv_freq = ROPE_BASE ** (-jnp.arange(0, HEAD, 2, dtype=jnp.float32) / HEAD)
    angles = positions.astype(jnp.float32).reshape(-1, 1) * inv_freq
    cos, sin = jnp.cos(angles), jnp.sin(angles)
    return jnp.concatenate([cos, cos], axis=-1), jnp.concatenate([-sin, sin], axis=-1)


def rope_round(vals, cos, sin):
    vals = vals.astype(jnp.bfloat16).astype(jnp.float32)
    return (vals * cos + pltpu.roll(vals, HEAD // 2, 1) * sin).astype(jnp.bfloat16)


def q_kernel(x_ref, w_ref, cos_ref, sin_ref, o_ref):
    rows, width = o_ref.shape
    step = 512

    @pl.loop(0, rows // step)
    def _(r):
        at = pl.ds(pl.multiple_of(r * step, step), step)
        x = x_ref[at, :]
        cos, sin = cos_ref[at, :], sin_ref[at, :]
        for c in range(0, width, 512):
            acc = jnp.dot(x, w_ref[:, c:c + 512], preferred_element_type=jnp.float32)
            for h in range(0, 512, HEAD):
                o_ref[at, c + h:c + h + HEAD] = rope_round(acc[:, h:h + HEAD], cos, sin)


def project_q(x, w, cos, sin, tile_m=512, tile_n=1024):
    m, d = x.shape
    n = w.shape[1]
    return pl.pallas_call(
        q_kernel,
        out_shape=jax.ShapeDtypeStruct((m, n), jnp.bfloat16),
        grid=(n // tile_n, m // tile_m),
        in_specs=[
            pl.BlockSpec((tile_m, d), lambda j, i: (i, 0)),
            pl.BlockSpec((d, tile_n), lambda j, i: (0, j)),
            pl.BlockSpec((tile_m, HEAD), lambda j, i: (i, 0)),
            pl.BlockSpec((tile_m, HEAD), lambda j, i: (i, 0)),
        ],
        out_specs=pl.BlockSpec((tile_m, tile_n), lambda j, i: (i, j)),
        compiler_params=pltpu.CompilerParams(vmem_limit_bytes=VMEM_LIMIT),
        cost_estimate=pl.CostEstimate(flops=2 * m * n * d, bytes_accessed=2 * (m * d + m * n + 4 * n * d), transcendentals=0),
        name="project_q",
    )(x, w, cos, sin)


def kv_kernel(x_ref, wk_ref, wv_ref, cos_ref, sin_ref, k_ref, v_ref):
    seqs, tok = v_ref.shape[0], v_ref.shape[2]

    x = x_ref[...]
    cos, sin = cos_ref[...], sin_ref[...]
    for c in range(0, wk_ref.shape[1], 256):
        acc = jnp.dot(x, wk_ref[:, c:c + 256], preferred_element_type=jnp.float32)
        for h in range(0, 256, HEAD):
            k_ref[:, :, c + h:c + h + HEAD] = rope_round(acc[:, h:h + HEAD], cos, sin).reshape(seqs, tok, HEAD)
        acc = jnp.dot(x, wv_ref[:, c:c + 256], preferred_element_type=jnp.float32)
        for s in range(seqs):
            v_ref[s, c:c + 256, :] = acc[s * tok:(s + 1) * tok, :].T.astype(jnp.bfloat16)


def project_kv(x, w_k, w_v, cos, sin, seq0, seqs, tok, tile_n=256):
    d, n = w_k.shape
    rows = seqs * tok
    assert seq0 % seqs == 0
    i0 = seq0 // seqs
    return pl.pallas_call(
        kv_kernel,
        out_shape=(
            jax.ShapeDtypeStruct((seqs, tok, n), jnp.bfloat16),
            jax.ShapeDtypeStruct((seqs, n, tok), jnp.bfloat16),
        ),
        grid=(n // tile_n,),
        in_specs=[
            pl.BlockSpec((rows, d), lambda j: (i0, 0)),
            pl.BlockSpec((d, tile_n), lambda j: (0, j)),
            pl.BlockSpec((d, tile_n), lambda j: (0, j)),
            pl.BlockSpec((rows, HEAD), lambda j: (i0, 0)),
            pl.BlockSpec((rows, HEAD), lambda j: (i0, 0)),
        ],
        out_specs=(
            pl.BlockSpec((seqs, tok, tile_n), lambda j: (0, 0, j)),
            pl.BlockSpec((seqs, tile_n, tok), lambda j: (0, j, 0)),
        ),
        compiler_params=pltpu.CompilerParams(vmem_limit_bytes=VMEM_LIMIT),
        cost_estimate=pl.CostEstimate(flops=4 * rows * n * d, bytes_accessed=2 * rows * d + 4 * n * d + 4 * rows * n, transcendentals=0),
        name="project_kv",
    )(x, w_k, w_v, cos, sin)


def attn_kernel(me_ref, q_ref, k_ref, v_ref, *rest):
    o_ref, s_even, s_odd = rest[-3:]
    me = me_ref[0]
    tok = q_ref.shape[1]
    heads = q_ref.shape[2] // HEAD
    per_kv = heads // (k_ref.shape[3] // HEAD)
    scale = HEAD ** -0.5 * LOG2E
    bufs = (s_even, s_odd)

    def scores(h, blocks, first_masked):
        buf = bufs[h % 2]
        q = q_ref[0, :, h * HEAD:(h + 1) * HEAD]
        top = jnp.full((8, tok), -jnp.inf, jnp.float32)
        kv = slice(h // per_kv * HEAD, (h // per_kv + 1) * HEAD)
        for j in range(blocks):
            s = lax.dot_general(k_ref[j, 0, :, kv], q, (((1,), (1,)), ((), ())), preferred_element_type=jnp.float32)
            if j >= first_masked:
                key = lax.broadcasted_iota(jnp.int32, (tok, tok), 0) + j * tok
                row = lax.broadcasted_iota(jnp.int32, (tok, tok), 1) + me * tok
                s = jnp.where(key <= row, s, -jnp.inf)
            buf[j * tok:(j + 1) * tok, :] = s
            top = jnp.maximum(top, jnp.max(s.reshape(tok // 8, 8, tok), axis=0))
        return jnp.max(top, axis=0, keepdims=True)

    def apply(h, blocks, top):
        buf = bufs[h % 2]
        shift = top * scale
        total = jnp.zeros((8, tok), jnp.float32)
        acc = None
        kv = slice(h // per_kv * HEAD, (h // per_kv + 1) * HEAD)
        for j in range(blocks):
            p = jnp.exp2(buf[j * tok:(j + 1) * tok, :] * scale - shift)
            total = total + jnp.sum(p.reshape(tok // 8, 8, tok), axis=0)
            part = jnp.dot(v_ref[j, 0, kv, :], p.astype(jnp.bfloat16), preferred_element_type=jnp.float32)
            acc = part if acc is None else acc + part
        out = acc * (1.0 / jnp.sum(total, axis=0, keepdims=True))
        o_ref[0, :, h * HEAD:(h + 1) * HEAD] = out.T.astype(jnp.bfloat16)

    def run(blocks, first_masked):
        tops = []
        for h in range(heads + 1):
            if h < heads:
                tops.append(scores(h, blocks, first_masked))
            if h > 0:
                apply(h - 1, blocks, tops[h - 1])

    n_dev = k_ref.shape[0]
    for pair in range(n_dev // 2):
        @pl.when(me // 2 == pair)
        def _():
            run(2 * pair + 2, 2 * pair)


def attention(me, q, k_all, v_all, seq0, after, kv_heads=2):
    n_dev, seqs, tok, kv_width = k_all.shape
    n_kv = kv_width // HEAD
    width = q.shape[2] // n_kv * kv_heads
    flops = 4 * seqs * tok * n_dev * tok * q.shape[2]
    return pl.pallas_call(
        attn_kernel,
        out_shape=jax.ShapeDtypeStruct((seqs, tok, q.shape[2]), jnp.bfloat16),
        grid_spec=pltpu.PrefetchScalarGridSpec(
            num_scalar_prefetch=1,
            grid=(seqs, n_kv // kv_heads),
            in_specs=[
                pl.BlockSpec((1, tok, width), lambda b, g, me: (b + seq0 if seq0 else b, 0, g)),
                pl.BlockSpec((n_dev, 1, tok, kv_heads * HEAD), lambda b, g, me: (0, b, 0, g)),
                pl.BlockSpec((n_dev, 1, kv_heads * HEAD, tok), lambda b, g, me: (0, b, g, 0)),
            ] + [pl.BlockSpec(memory_space=pl.ANY)] * len(after),
            out_specs=pl.BlockSpec((1, tok, width), lambda b, g, me: (b, 0, g)),
            scratch_shapes=[pltpu.VMEM((n_dev * tok, tok), jnp.float32)] * 2,
        ),
        compiler_params=pltpu.CompilerParams(vmem_limit_bytes=VMEM_LIMIT),
        cost_estimate=pl.CostEstimate(flops=flops, bytes_accessed=4 * k_all.size + 4 * seqs * tok * q.shape[2], transcendentals=0),
        name="attention",
    )(me, q, k_all, v_all, *after)


def o_kernel(o_ref, w_ref, x_ref, *rest):
    y_ref = rest[-1]
    a = o_ref[...]
    for c in range(0, w_ref.shape[1], 256):
        acc = jnp.dot(a, w_ref[:, c:c + 256], preferred_element_type=jnp.float32)
        y_ref[:, c:c + 256] = (x_ref[:, c:c + 256].astype(jnp.float32) + acc).astype(jnp.bfloat16)


def project_o(o, w, x, y, row0, tile_n=512):
    rows, n_in = o.shape
    m, d = x.shape
    assert row0 % rows == 0
    i0 = row0 // rows
    specs = [
        pl.BlockSpec((rows, n_in), lambda j: (0, 0)),
        pl.BlockSpec((n_in, tile_n), lambda j: (0, j)),
        pl.BlockSpec((rows, tile_n), lambda j: (i0, j)),
    ]
    args = [o, w, x]
    alias = {}
    if y is not None:
        specs.append(pl.BlockSpec(memory_space=pl.ANY))
        args.append(y)
        alias = {3: 0}
    return pl.pallas_call(
        o_kernel,
        out_shape=jax.ShapeDtypeStruct((m, d), jnp.bfloat16),
        grid=(d // tile_n,),
        in_specs=specs,
        out_specs=pl.BlockSpec((rows, tile_n), lambda j: (i0, j)),
        input_output_aliases=alias,
        compiler_params=pltpu.CompilerParams(vmem_limit_bytes=VMEM_LIMIT),
        cost_estimate=pl.CostEstimate(flops=2 * rows * n_in * d, bytes_accessed=2 * (n_in * d + rows * n_in + 2 * rows * d), transcendentals=0),
        name="project_o",
    )(*args)


def solution(mesh):
    def per_device(hidden, positions, w_q, w_k, w_v, w_o):
        seqs, tok, d = hidden.shape
        x = hidden.reshape(seqs * tok, d)
        w_q = w_q.reshape(d, -1)
        w_k = w_k.reshape(d, -1)
        w_v = lax.optimization_barrier((w_v, w_k))[0].reshape(d, -1)
        w_o = w_o.reshape(-1, d)
        cos, sin = rope_tables(positions)
        me = lax.axis_index('cp').astype(jnp.int32).reshape(1)
        gathered = []
        seq0 = 0
        for n in CHUNKS:
            k, v = project_kv(x, w_k, w_v, cos, sin, seq0, n, tok)
            gathered.append((lax.all_gather(k, 'cp', axis=0), lax.all_gather(v, 'cp', axis=0)))
            seq0 += n
        q = project_q(x, w_q, cos, sin).reshape(seqs, tok, -1)
        y = None
        seq0 = 0
        for n, (k_all, v_all) in zip(CHUNKS, gathered):
            o = attention(me, q, k_all, v_all, seq0, () if y is None else (y,))
            y = project_o(o.reshape(n * tok, -1), w_o, x, y, seq0 * tok)
            seq0 += n
        return y.reshape(seqs, tok, d)

    rep_spec = P(None, None, None)
    return jax.shard_map(per_device, mesh=mesh, in_specs=(P('dp', 'cp', None), P('dp', 'cp'), rep_spec, rep_spec, rep_spec, rep_spec), out_specs=P('dp', 'cp', None), check_vma=False)
```

```python
import functools

import jax
import jax.numpy as jnp
from jax import lax
from jax.experimental import pallas as pl
from jax.experimental.pallas import tpu as pltpu
from jax.sharding import PartitionSpec as P

ROPE_BASE = 500000.0
HEAD = 128
LOG2E = 1.4426950408889634
VMEM_LIMIT = 60 * 1024 * 1024
CHUNKS = 4


def rope_tables(positions):
    inv_freq = ROPE_BASE ** (-jnp.arange(0, HEAD, 2, dtype=jnp.float32) / HEAD)
    angles = positions.astype(jnp.float32).reshape(-1, 1) * inv_freq
    cos, sin = jnp.cos(angles), jnp.sin(angles)
    return jnp.concatenate([cos, cos], axis=-1), jnp.concatenate([-sin, sin], axis=-1)


def rope_round(vals, cos, sin):
    vals = vals.astype(jnp.bfloat16).astype(jnp.float32)
    return (vals * cos + pltpu.roll(vals, HEAD // 2, 1) * sin).astype(jnp.bfloat16)


def q_kernel(x_ref, w_ref, cos_ref, sin_ref, o_ref):
    rows, width = o_ref.shape
    step = 512

    @pl.loop(0, rows // step)
    def _(r):
        at = pl.ds(pl.multiple_of(r * step, step), step)
        x = x_ref[at, :]
        cos, sin = cos_ref[at, :], sin_ref[at, :]
        for c in range(0, width, 512):
            acc = jnp.dot(x, w_ref[:, c:c + 512], preferred_element_type=jnp.float32)
            for h in range(0, 512, HEAD):
                o_ref[at, c + h:c + h + HEAD] = rope_round(acc[:, h:h + HEAD], cos, sin)


def project_q(x, w, cos, sin, tile_m=512, tile_n=1024):
    m, d = x.shape
    n = w.shape[1]
    return pl.pallas_call(
        q_kernel,
        out_shape=jax.ShapeDtypeStruct((m, n), jnp.bfloat16),
        grid=(n // tile_n, m // tile_m),
        in_specs=[
            pl.BlockSpec((tile_m, d), lambda j, i: (i, 0)),
            pl.BlockSpec((d, tile_n), lambda j, i: (0, j)),
            pl.BlockSpec((tile_m, HEAD), lambda j, i: (i, 0)),
            pl.BlockSpec((tile_m, HEAD), lambda j, i: (i, 0)),
        ],
        out_specs=pl.BlockSpec((tile_m, tile_n), lambda j, i: (i, j)),
        compiler_params=pltpu.CompilerParams(vmem_limit_bytes=VMEM_LIMIT),
        cost_estimate=pl.CostEstimate(flops=2 * m * n * d, bytes_accessed=2 * (m * d + m * n + 4 * n * d), transcendentals=0),
        name="project_q",
    )(x, w, cos, sin)


def kv_kernel(x_ref, wk_ref, wv_ref, cos_ref, sin_ref, *out_refs):
    seqs, tok = out_refs[1].shape[0], out_refs[1].shape[2]

    def run(k_ref, v_ref):
        x = x_ref[...]
        cos, sin = cos_ref[...], sin_ref[...]
        for c in range(0, wk_ref.shape[1], 256):
            acc = jnp.dot(x, wk_ref[:, c:c + 256], preferred_element_type=jnp.float32)
            for h in range(0, 256, HEAD):
                k_ref[:, :, c + h:c + h + HEAD] = rope_round(acc[:, h:h + HEAD], cos, sin).reshape(seqs, tok, HEAD)
            acc = jnp.dot(x, wv_ref[:, c:c + 256], preferred_element_type=jnp.float32)
            for s in range(seqs):
                v_ref[s, c:c + 256, :] = acc[s * tok:(s + 1) * tok, :].T.astype(jnp.bfloat16)

    if len(out_refs) == 2:
        run(*out_refs)
    else:
        for c in range(len(out_refs) // 2):
            pl.when(pl.program_id(0) == c)(functools.partial(run, *out_refs[2 * c:2 * c + 2]))


def project_kv(x, w_k, w_v, cos, sin, chunk0, chunks, seqs, tok, tile_n=256):
    d, n = w_k.shape
    rows = seqs * tok
    tiles = n // tile_n

    def tile_of(chunk):
        return lambda i, j: jnp.where(i < chunk, 0, jnp.where(i == chunk, j, tiles - 1))

    def specs_of(chunk):
        at = tile_of(chunk)
        return [
            pl.BlockSpec((seqs, tok, tile_n), lambda i, j: (0, 0, at(i, j))),
            pl.BlockSpec((seqs, tile_n, tok), lambda i, j: (0, at(i, j), 0)),
        ]

    outs = pl.pallas_call(
        kv_kernel,
        out_shape=[
            jax.ShapeDtypeStruct((seqs, tok, n), jnp.bfloat16),
            jax.ShapeDtypeStruct((seqs, n, tok), jnp.bfloat16),
        ] * chunks,
        grid=(chunks, tiles),
        in_specs=[
            pl.BlockSpec((rows, d), lambda i, j: (i + chunk0, 0)),
            pl.BlockSpec((d, tile_n), lambda i, j: (0, j)),
            pl.BlockSpec((d, tile_n), lambda i, j: (0, j)),
            pl.BlockSpec((rows, HEAD), lambda i, j: (i + chunk0, 0)),
            pl.BlockSpec((rows, HEAD), lambda i, j: (i + chunk0, 0)),
        ],
        out_specs=[spec for chunk in range(chunks) for spec in specs_of(chunk)],
        compiler_params=pltpu.CompilerParams(vmem_limit_bytes=VMEM_LIMIT),
        cost_estimate=pl.CostEstimate(flops=4 * chunks * rows * n * d, bytes_accessed=2 * chunks * rows * d + 4 * chunks * n * d + 4 * chunks * rows * n, transcendentals=0),
        name="project_kv",
    )(x, w_k, w_v, cos, sin)
    return [(outs[2 * c], outs[2 * c + 1]) for c in range(chunks)]


def attn_kernel(me_ref, q_ref, k_ref, v_ref, *rest):
    o_ref, s_even, s_odd = rest[-3:]
    me = me_ref[0]
    tok = q_ref.shape[1]
    heads = q_ref.shape[2] // HEAD
    per_kv = heads // (k_ref.shape[3] // HEAD)
    scale = HEAD ** -0.5 * LOG2E
    bufs = (s_even, s_odd)

    def scores(h, blocks, first_masked):
        buf = bufs[h % 2]
        q = q_ref[0, :, h * HEAD:(h + 1) * HEAD]
        top = jnp.full((8, tok), -jnp.inf, jnp.float32)
        kv = slice(h // per_kv * HEAD, (h // per_kv + 1) * HEAD)
        for j in range(blocks):
            s = lax.dot_general(k_ref[j, 0, :, kv], q, (((1,), (1,)), ((), ())), preferred_element_type=jnp.float32) * scale
            if j >= first_masked:
                key = lax.broadcasted_iota(jnp.int32, (tok, tok), 0) + j * tok
                row = lax.broadcasted_iota(jnp.int32, (tok, tok), 1) + me * tok
                s = jnp.where(key <= row, s, -jnp.inf)
            buf[j * tok:(j + 1) * tok, :] = s
            top = jnp.maximum(top, jnp.max(s.reshape(tok // 8, 8, tok), axis=0))
        return jnp.max(top, axis=0, keepdims=True)

    def apply(h, blocks, top):
        buf = bufs[h % 2]
        total = jnp.zeros((8, tok), jnp.float32)
        acc = None
        kv = slice(h // per_kv * HEAD, (h // per_kv + 1) * HEAD)
        for j in range(blocks):
            p = jnp.exp2(buf[j * tok:(j + 1) * tok, :] - top)
            total = total + jnp.sum(p.reshape(tok // 8, 8, tok), axis=0)
            part = jnp.dot(v_ref[j, 0, kv, :], p.astype(jnp.bfloat16), preferred_element_type=jnp.float32)
            acc = part if acc is None else acc + part
        out = acc * (1.0 / jnp.sum(total, axis=0, keepdims=True))
        o_ref[0, :, h * HEAD:(h + 1) * HEAD] = out.T.astype(jnp.bfloat16)

    def run(blocks, first_masked):
        tops = []
        for h in range(heads + 1):
            if h < heads:
                tops.append(scores(h, blocks, first_masked))
            if h > 0:
                apply(h - 1, blocks, tops[h - 1])

    n_dev = k_ref.shape[0]
    low = 0
    for high in [*range(n_dev - 6, n_dev - 1, 2), n_dev - 1]:
        pl.when((me >= low) & (me <= high))(functools.partial(run, high + 1, low))
        low = high + 1


def attention(me, q, k_all, v_all, seq0, after, kv_heads=2):
    n_dev, seqs, tok, kv_width = k_all.shape
    n_kv = kv_width // HEAD
    width = q.shape[2] // n_kv * kv_heads
    flops = 4 * seqs * tok * n_dev * tok * q.shape[2]
    return pl.pallas_call(
        attn_kernel,
        out_shape=jax.ShapeDtypeStruct((seqs, tok, q.shape[2]), jnp.bfloat16),
        grid_spec=pltpu.PrefetchScalarGridSpec(
            num_scalar_prefetch=1,
            grid=(seqs, n_kv // kv_heads),
            in_specs=[
                pl.BlockSpec((1, tok, width), lambda b, g, me: (b + seq0 if seq0 else b, 0, g)),
                pl.BlockSpec((n_dev, 1, tok, kv_heads * HEAD), lambda b, g, me: (0, b, 0, g)),
                pl.BlockSpec((n_dev, 1, kv_heads * HEAD, tok), lambda b, g, me: (0, b, g, 0)),
            ] + [pl.BlockSpec(memory_space=pl.ANY)] * len(after),
            out_specs=pl.BlockSpec((1, tok, width), lambda b, g, me: (b, 0, g)),
            scratch_shapes=[pltpu.VMEM((n_dev * tok, tok), jnp.float32)] * 2,
        ),
        compiler_params=pltpu.CompilerParams(vmem_limit_bytes=VMEM_LIMIT),
        cost_estimate=pl.CostEstimate(flops=flops, bytes_accessed=4 * k_all.size + 4 * seqs * tok * q.shape[2], transcendentals=0),
        name="attention",
    )(me, q, k_all, v_all, *after)


def o_kernel(o_ref, w_ref, x_ref, *rest):
    y_ref = rest[-1]
    a = o_ref[...]
    for c in range(0, w_ref.shape[1], 256):
        acc = jnp.dot(a, w_ref[:, c:c + 256], preferred_element_type=jnp.float32)
        y_ref[:, c:c + 256] = (x_ref[:, c:c + 256].astype(jnp.float32) + acc).astype(jnp.bfloat16)


def project_o(o, w, x, y, row0, tile_n=512):
    rows, n_in = o.shape
    m, d = x.shape
    assert row0 % rows == 0
    i0 = row0 // rows
    specs = [
        pl.BlockSpec((rows, n_in), lambda j: (0, 0)),
        pl.BlockSpec((n_in, tile_n), lambda j: (0, j)),
        pl.BlockSpec((rows, tile_n), lambda j: (i0, j)),
    ]
    args = [o, w, x]
    alias = {}
    if y is not None:
        specs.append(pl.BlockSpec(memory_space=pl.ANY))
        args.append(y)
        alias = {3: 0}
    return pl.pallas_call(
        o_kernel,
        out_shape=jax.ShapeDtypeStruct((m, d), jnp.bfloat16),
        grid=(d // tile_n,),
        in_specs=specs,
        out_specs=pl.BlockSpec((rows, tile_n), lambda j: (i0, j)),
        input_output_aliases=alias,
        compiler_params=pltpu.CompilerParams(vmem_limit_bytes=VMEM_LIMIT),
        cost_estimate=pl.CostEstimate(flops=2 * rows * n_in * d, bytes_accessed=2 * (n_in * d + rows * n_in + 2 * rows * d), transcendentals=0),
        name="project_o",
    )(*args)


def solution(mesh):
    def per_device(hidden, positions, w_q, w_k, w_v, w_o):
        seqs, tok, d = hidden.shape
        x = hidden.reshape(seqs * tok, d)
        w_q = w_q.reshape(d, -1)
        w_k = w_k.reshape(d, -1)
        w_v = lax.optimization_barrier((w_v, w_k))[0].reshape(d, -1)
        w_o = w_o.reshape(-1, d)
        cos, sin = rope_tables(positions)
        me = lax.axis_index('cp').astype(jnp.int32).reshape(1)
        n = seqs // CHUNKS
        pairs = project_kv(x, w_k, w_v, cos, sin, 0, 1, n, tok)
        pairs += project_kv(x, w_k, w_v, cos, sin, 1, CHUNKS - 1, n, tok)
        gathered = [(lax.all_gather(k, 'cp', axis=0), lax.all_gather(v, 'cp', axis=0)) for k, v in pairs]
        q = project_q(x, w_q, cos, sin).reshape(seqs, tok, -1)
        y = None
        for c, (k_all, v_all) in enumerate(gathered):
            o = attention(me, q, k_all, v_all, c * n, () if y is None else (y,))
            y = project_o(o.reshape(n * tok, -1), w_o, x, y, c * n * tok)
        return y.reshape(seqs, tok, d)

    rep_spec = P(None, None, None)
    return jax.shard_map(per_device, mesh=mesh, in_specs=(P('dp', 'cp', None), P('dp', 'cp'), rep_spec, rep_spec, rep_spec, rep_spec), out_specs=P('dp', 'cp', None), check_vma=False)
```
